32 devices in a mesh: frame: 4 (over x, core), seq: 8 (over z, y).
Axes of the slice: x: 2, y: 2, z: 4, core: 2. Of those that a mesh axis runs over, the one named last changes fastest.
Arguments:
- vit_states: bfloat16 [64, 256, 1280], P(('frame', 'seq')), may hold values from -6 to 6
- frame_slot: int32 [32], replicated, may hold values from 0 to 63, as said below
- patch_count: int32 [32], replicated, may hold values from 208 to 256, as said below
- vis_start: int32 [32], replicated, may hold values from 0 to 4095, as said below
- text_embed: bfloat16 [128, 32, 4096], P(None, ('frame', 'seq')), may hold values from -6 to 6
- vit_ln_gain: float32 [1280], replicated, may hold values from 0.25 to 1.75
- vit_ln_bias: float32 [1280], replicated, may hold values from -1.5 to 1.5
- vit_qkv_w: bfloat16 [1280, 3840], P('seq'), may hold values from -0.15625 to 0.15625
- vit_qkv_b: float32 [3840], replicated, may hold values from -1.5 to 1.5
- vit_out_w: bfloat16 [1280, 1280], P('seq'), may hold values from -0.15625 to 0.15625
- vit_out_b: float32 [1280], replicated, may hold values from -1.5 to 1.5
- proj_w: bfloat16 [1280, 4096], replicated, may hold values from -0.15625 to 0.15625
- proj_b: float32 [4096], replicated, may hold values from -1.5 to 1.5
- attn_gain: float32 [4096], replicated, may hold values from 0.25 to 1.75
- wq: bfloat16 [4096, 2048], P(None, 'frame'), may hold values from -0.09375 to 0.09375
- wk: bfloat16 [4096, 1024], P(None, 'frame'), may hold values from -0.09375 to 0.09375
- wv: bfloat16 [4096, 1024], P(None, 'frame'), may hold values from -0.09375 to 0.09375
- wo: bfloat16 [2048, 4096], P('frame'), may hold values from -0.125 to 0.125
Outputs:
- mixed: bfloat16 [128, 32, 4096], P(None, ('frame', 'seq'))
The draws below stay inside these ranges and needn't reach their ends.
Inputs may be any that keep to these rules, and one draw needn't show every extreme that they name: Frame t sits in slot frame_slot[t]; slot k of the device with index d (axes frame then seq) is d * 2 + k; no slot holds two frames. The two devices with frame indices 2i and 2i+1 and the same seq index hold exactly two frames between them; some device holds 2 frames. `patch_count`: A multiple of 4; some frame has 256 patches. Frame t's patch_count[t] / 4 visual positions start at vis_start[t] and lie within positions t * 128 to (t + 1) * 128 - 1.
All inputs are finite; a program needn't handle non-finite values.
Results may differ from the reference program's by a relative error of at most 0.015.
Values may be sent and summed in bfloat16 or wider, within the bound.
A program may use at most 128 MiB of HBM per device.

```python
import math
import jax
import jax.numpy as jnp
from jax import lax

VW = 1280
VHEADS = 16
MODEL_WIDTH = 4096
QUERY_HEADS_HALF = 16
KEY_VALUE_HEADS = 8
HEAD_WIDTH = 128
FRAME_MAX = 256
SLOTS = 2
TOK_OWN = 128
VIS_MAX = 64
N_FRAME = 4
N_SEQ = 8
DEVICES = 32


def frame_spans(key):
    inner_key = jax.random.fold_in(key, 5)
    count_key, place_key = jax.random.split(inner_key)
    lowest = VIS_MAX - VIS_MAX // 5
    tokens = jax.random.randint(count_key, (DEVICES,), lowest, VIS_MAX + 1).astype(jnp.int32)
    tokens = tokens.at[0].set(VIS_MAX)
    spare = TOK_OWN - tokens
    offsets = jax.random.randint(place_key, (DEVICES,), 0, spare + 1).astype(jnp.int32)
    starts = jnp.arange(DEVICES).astype(jnp.int32) * TOK_OWN + offsets
    return (tokens * 4, starts)


def draw_patch_count(key, part):
    counts, starts = frame_spans(key)
    return counts


def draw_vis_start(key, part):
    counts, starts = frame_spans(key)
    return starts


def draw_frame_slot(key, part):
    pairs_n = DEVICES // 2
    order_key, slot_key = jax.random.split(jax.random.fold_in(key, 3))
    frames_perm = jax.random.permutation(order_key, DEVICES).astype(jnp.int32)
    scores = jax.random.randint(slot_key, (pairs_n, 4), 0, 1 << 20) * 4 + jnp.arange(4).astype(jnp.int32)[None, :]
    chosen = jnp.argsort(scores, axis=1)[:, :2].astype(jnp.int32)
    chosen = chosen.at[0].set(jnp.array([0, 1], jnp.int32))
    earlier_slot = jnp.min(chosen, axis=1)
    later_slot = jnp.max(chosen, axis=1)
    pair_ids = jnp.arange(pairs_n).astype(jnp.int32)
    low_device = pair_ids // N_SEQ * 2 * N_SEQ + pair_ids % N_SEQ
    first_slots = (low_device + earlier_slot // 2 * N_SEQ) * 2 + earlier_slot % 2
    second_slots = (low_device + later_slot // 2 * N_SEQ) * 2 + later_slot % 2
    result = jnp.zeros((DEVICES,), jnp.int32)
    result = result.at[frames_perm[0::2]].set(first_slots)
    result = result.at[frames_perm[1::2]].set(second_slots)
    return result


def level_of(own_key, dims, shards, smallest, largest):
    def one(position, shards_of):
        steps = jax.random.uniform(jax.random.fold_in(jax.random.fold_in(own_key, 6), position), (shards_of,), jnp.float32, smallest / len(shards), largest / len(shards))
        return jnp.repeat(jnp.exp(steps), dims[position] // shards_of).reshape((-1,) + (1,) * (len(dims) - position - 1))

    gain = one(*shards[0])
    for cut in shards[1:]:
        gain = gain * one(*cut)
    return gain


def normal_values(stream_key, extent, scale, limit, cuts=(), held_as=jnp.bfloat16):
    values = jax.random.normal(stream_key, extent, jnp.float32) * scale
    if len(cuts) > 0:
        values = level_of(stream_key, extent, cuts, -0.22, 0.18) * values
    return jnp.clip(values, min=-limit, max=limit).astype(held_as)


def setup_inputs(seed: int = 0) -> dict:
    key_list = jax.random.split(jax.random.key(seed), 19)
    return {
        "vit_states": normal_values(key_list[0], (DEVICES * SLOTS, FRAME_MAX, VW), 1.0, 6.0, ((0, 32),)),
        "frame_slot": draw_frame_slot(jax.random.fold_in(key_list[18], 71), 0),
        "patch_count": draw_patch_count(jax.random.fold_in(key_list[18], 71), 0),
        "vis_start": draw_vis_start(jax.random.fold_in(key_list[18], 71), 0),
        "text_embed": normal_values(key_list[4], (TOK_OWN, DEVICES, MODEL_WIDTH), 1.0, 6.0, ((1, 32),)),
        "vit_ln_gain": jnp.clip(1.0 + 0.15 * jax.random.normal(key_list[5], (VW,), jnp.float32), 0.25, 1.75),
        "vit_ln_bias": normal_values(key_list[6], (VW,), 0.3, 1.5, (), jnp.float32),
        "vit_qkv_w": normal_values(key_list[7], (VW, 3 * VW), VW ** -0.5, 0.15625, ((0, 8),)),
        "vit_qkv_b": normal_values(key_list[8], (3 * VW,), 0.3, 1.5, (), jnp.float32),
        "vit_out_w": normal_values(key_list[9], (VW, VW), VW ** -0.5, 0.15625, ((0, 8),)),
        "vit_out_b": normal_values(key_list[10], (VW,), 0.3, 1.5, (), jnp.float32),
        "proj_w": normal_values(key_list[11], (VW, MODEL_WIDTH), VW ** -0.5, 0.15625),
        "proj_b": normal_values(key_list[12], (MODEL_WIDTH,), 0.3, 1.5, (), jnp.float32),
        "attn_gain": jnp.clip(1.0 + 0.15 * jax.random.normal(key_list[13], (MODEL_WIDTH,), jnp.float32), 0.25, 1.75),
        "wq": normal_values(key_list[14], (MODEL_WIDTH, QUERY_HEADS_HALF * HEAD_WIDTH), MODEL_WIDTH ** -0.5, 0.09375, ((1, 4),)),
        "wk": normal_values(key_list[15], (MODEL_WIDTH, KEY_VALUE_HEADS * HEAD_WIDTH), MODEL_WIDTH ** -0.5, 0.09375, ((1, 4),)),
        "wv": normal_values(key_list[16], (MODEL_WIDTH, KEY_VALUE_HEADS * HEAD_WIDTH), MODEL_WIDTH ** -0.5, 0.09375, ((1, 4),)),
        "wo": normal_values(key_list[17], (QUERY_HEADS_HALF * HEAD_WIDTH, MODEL_WIDTH), (QUERY_HEADS_HALF * HEAD_WIDTH) ** -0.5, 0.125, ((0, 4),)),
    }


rope_theta = 500000.0
vit_epsilon = 1e-06
norm_epsilon = 1e-05
masked_score = -1e+30

def apply_rotary(values, rotary_angles):
    half_width = values.shape[-1] // 2
    first_half = values[..., :half_width]
    second_half = values[..., half_width:]
    cosine = jnp.cos(rotary_angles)
    sine_part = jnp.sin(rotary_angles)
    return jnp.concatenate([first_half * cosine - second_half * sine_part, second_half * cosine + first_half * sine_part], axis=-1)

def rope_angles(positions, head_size):
    exponents = jnp.arange(0, head_size, 2).astype(jnp.float32) / head_size
    inverse = jnp.power(jnp.float32(rope_theta), -exponents)
    return positions.astype(jnp.float32)[:, None] * inverse[None, :]

def vit_frame(states, patches, ln_gain, ln_bias, qkv_weight, qkv_bias, out_weight, out_bias):
    frame_max = states.shape[0]
    width_vit = states.shape[1]
    states_wide = states.astype(jnp.float32)
    average = lax.optimization_barrier(jnp.mean(states_wide, axis=1, keepdims=True))
    centred = states_wide - average
    spread = lax.optimization_barrier(jnp.mean(centred * centred, axis=1, keepdims=True))
    normed_states = (centred * lax.rsqrt(spread + vit_epsilon) * ln_gain + ln_bias).astype(jnp.bfloat16)
    projected = (jnp.dot(normed_states, qkv_weight, preferred_element_type=jnp.float32) + qkv_bias).astype(jnp.bfloat16)
    head_size = width_vit // VHEADS
    shaped = projected.reshape(frame_max, 3, VHEADS, head_size).astype(jnp.float32)
    scores = jnp.einsum('qhd,khd->hqk', shaped[:, 0], shaped[:, 1]) / math.sqrt(head_size)
    key_live = jnp.arange(frame_max).astype(jnp.int32) < patches
    scores = jnp.where(key_live[None, None, :], scores, masked_score)
    highest = lax.optimization_barrier(jnp.max(scores, axis=-1, keepdims=True))
    weights = jnp.exp(scores - highest)
    probabilities = (weights / lax.optimization_barrier(jnp.sum(weights, axis=-1, keepdims=True))).astype(jnp.bfloat16)
    context = jnp.einsum('hqk,khd->qhd', probabilities.astype(jnp.float32), shaped[:, 2]).astype(jnp.bfloat16)
    attended = jnp.dot(context.reshape(frame_max, width_vit), out_weight, preferred_element_type=jnp.float32)
    hidden = (states_wide + attended + out_bias).astype(jnp.bfloat16)
    return lax.optimization_barrier(jnp.mean(hidden.astype(jnp.float32).reshape(frame_max // 4, 4, width_vit), axis=1)).astype(jnp.bfloat16)

def reference(vit_states, frame_slot, patch_count, vis_start, text_embed, vit_ln_gain, vit_ln_bias, vit_qkv_w, vit_qkv_b, vit_out_w, vit_out_b, proj_w, proj_b, attn_gain, wq, wk, wv, wo):
    frame_states = vit_states[frame_slot]

    def encode(operands):
        states, patches = operands
        pooled = vit_frame(states, patches, vit_ln_gain, vit_ln_bias, vit_qkv_w, vit_qkv_b, vit_out_w, vit_out_b)
        return (jnp.dot(pooled, proj_w, preferred_element_type=jnp.float32) + proj_b).astype(jnp.bfloat16)
    visual = lax.map(encode, (frame_states, patch_count))
    sequence_length = TOK_OWN * DEVICES
    positions = jnp.arange(sequence_length).astype(jnp.int32)
    token_frame = positions // TOK_OWN
    within = positions - vis_start[token_frame]
    is_visual = (within >= 0) & (within < patch_count[token_frame] // 4)
    within_clip = jnp.clip(within, 0, VIS_MAX - 1)
    visual_rows = visual[token_frame, within_clip]
    merged = jnp.where(is_visual[:, None], visual_rows, text_embed.reshape(sequence_length, MODEL_WIDTH))
    merged_wide = merged.astype(jnp.float32)
    normed_states = (merged_wide * lax.rsqrt(lax.optimization_barrier(jnp.mean(merged_wide * merged_wide, axis=1, keepdims=True)) + norm_epsilon) * attn_gain).astype(jnp.bfloat16)
    rotary_angles = rope_angles(positions, HEAD_WIDTH)[:, None, :]
    query_matrix = apply_rotary(jnp.dot(normed_states, wq, preferred_element_type=jnp.float32).reshape(sequence_length, QUERY_HEADS_HALF, HEAD_WIDTH), rotary_angles).astype(jnp.bfloat16)
    keys_complete = apply_rotary(jnp.dot(normed_states, wk, preferred_element_type=jnp.float32).reshape(sequence_length, KEY_VALUE_HEADS, HEAD_WIDTH), rotary_angles).astype(jnp.bfloat16)
    values_complete = jnp.dot(normed_states, wv, preferred_element_type=jnp.float32).astype(jnp.bfloat16).reshape(sequence_length, KEY_VALUE_HEADS, HEAD_WIDTH)
    keys_wide = keys_complete.astype(jnp.float32)
    values_wide = values_complete.astype(jnp.float32)
    grouped_rows = query_matrix.reshape(sequence_length, KEY_VALUE_HEADS, QUERY_HEADS_HALF // KEY_VALUE_HEADS, HEAD_WIDTH)
    query_rows = 128

    def attend(block_index):
        offset = block_index * query_rows
        query_block = lax.dynamic_slice_in_dim(grouped_rows, offset, query_rows, 0).astype(jnp.float32)
        scores = jnp.einsum('qkgd,nkd->kgqn', query_block, keys_wide) / math.sqrt(HEAD_WIDTH)
        query_positions = offset + jnp.arange(query_rows).astype(jnp.int32)
        allowed = positions[None, :] <= query_positions[:, None]
        scores = jnp.where(allowed[None, None], scores, masked_score)
        highest = lax.optimization_barrier(jnp.max(scores, axis=-1, keepdims=True))
        weights = jnp.where(allowed[None, None], jnp.exp(scores - highest), 0.0)
        denominator = lax.optimization_barrier(jnp.sum(weights, axis=-1))
        numerator = jnp.einsum('kgqn,nkd->kgqd', weights.astype(jnp.bfloat16).astype(jnp.float32), values_wide)
        context_block = (numerator / denominator[..., None]).astype(jnp.bfloat16)
        return jnp.transpose(context_block, (2, 0, 1, 3)).reshape(query_rows, QUERY_HEADS_HALF * HEAD_WIDTH)
    context = lax.map(attend, jnp.arange(sequence_length // query_rows).astype(jnp.int32)).reshape(sequence_length, QUERY_HEADS_HALF * HEAD_WIDTH)
    group_width = QUERY_HEADS_HALF * HEAD_WIDTH // N_FRAME
    summed = jnp.zeros((sequence_length, MODEL_WIDTH), jnp.float32)
    for head_group in range(N_FRAME):
        columns = context[:, head_group * group_width:(head_group + 1) * group_width]
        partial_sum = jnp.dot(columns, wo[head_group * group_width:(head_group + 1) * group_width], preferred_element_type=jnp.float32)
        rounded = lax.optimization_barrier(partial_sum.astype(jnp.bfloat16))
        summed = summed + rounded.astype(jnp.float32)
    return summed.astype(jnp.bfloat16).reshape(TOK_OWN, DEVICES, MODEL_WIDTH)
```

```python
import functools
import math

import jax
import jax.numpy as jnp
from jax import lax
from jax.experimental import pallas as pl
from jax.experimental.pallas import tpu as pltpu
from jax.sharding import PartitionSpec as P

VHEADS = 16
HEAD_WIDTH = 128

rope_theta = 500000.0
vit_epsilon = 1e-06
norm_epsilon = 1e-05
masked_score = -1e30
LOG2E = math.log2(math.e)


def dot32(a, b):
    return jnp.dot(a, b, preferred_element_type=jnp.float32)


def from_relative(value, dx, dc):
    n = lax.axis_size("frame")
    chips = n // 2
    pairs = []
    for dst in range(n):
        src = ((dst // 2 + dx) % chips) * 2 + ((dst % 2) ^ dc)
        pairs.append((src, dst))
    return lax.ppermute(value, "frame", pairs)


def gather_relative(value):
    chips = lax.axis_size("frame") // 2
    out = []
    for dx in range(chips):
        same = value if dx == 0 else from_relative(value, dx, 0)
        out.append(same)
        out.append(from_relative(same, 0, 1))
    return out


def to_absolute(parts):
    n = len(parts)
    chips = n // 2
    me = lax.axis_index("frame")
    stack = jnp.stack(parts)
    out = []
    for g in range(n):
        dx = jnp.mod(g // 2 - me // 2, chips)
        dc = (g % 2) ^ (me % 2)
        out.append(lax.dynamic_index_in_dim(stack, dx * 2 + dc, 0, keepdims=False))
    return jnp.stack(out)


def vit_kernel(count_ref, q_ref, k_ref, v_ref, o_ref, *, heads, head_size):
    frame = pl.program_id(0)
    rows, width = q_ref.shape[1], q_ref.shape[2]
    q = q_ref[0]
    k = k_ref[0]
    v = v_ref[0]
    count = count_ref[frame]
    column = lax.broadcasted_iota(jnp.int32, (rows, rows), 1)
    live = column < count
    lane = lax.broadcasted_iota(jnp.int32, (rows, width), 1)
    zero = jnp.zeros((), q.dtype)
    total = jnp.zeros((rows, width), jnp.float32)
    for h in range(heads):
        mine = (lane >= h * head_size) & (lane < (h + 1) * head_size)
        qh = jnp.where(mine, q, zero)
        s = lax.dot_general(qh, k, (((1,), (1,)), ((), ())), preferred_element_type=jnp.float32)
        s = jnp.where(live, s * (1.0 / math.sqrt(head_size)), masked_score)
        e = jnp.exp(s - jnp.max(s, axis=1, keepdims=True))
        p = (e / jnp.sum(e, axis=1, keepdims=True)).astype(jnp.bfloat16)
        vh = jnp.where(mine, v, zero)
        total = total + dot32(p, vh)
    context = total.astype(jnp.bfloat16)
    out_rows = o_ref.shape[1]
    pr = lax.broadcasted_iota(jnp.int32, (out_rows, rows), 0)
    pc = lax.broadcasted_iota(jnp.int32, (out_rows, rows), 1)
    pool = jnp.where(pc // 4 == pr, 0.25, 0.0).astype(jnp.bfloat16)
    o_ref[0] = dot32(pool, context).astype(jnp.bfloat16)


def vit_attention(counts, q, k, v, heads, head_size):
    frames, rows, width = q.shape
    block = pl.BlockSpec((1, rows, width), lambda i: (i, 0, 0))
    return pl.pallas_call(
        functools.partial(vit_kernel, heads=heads, head_size=head_size),
        grid=(frames,),
        in_specs=[pl.BlockSpec(memory_space=pltpu.SMEM), block, block, block],
        out_specs=pl.BlockSpec((1, rows // 4, width), lambda i: (i, 0, 0)),
        out_shape=jax.ShapeDtypeStruct((frames, rows // 4, width), jnp.bfloat16),
        name="vit_attention",
    )(counts, q, k, v)


def text_kernel(q_ref, kv_ref, o_ref, *, kv_heads, group, sub, seq_step):
    frames_n, own_rows = q_ref.shape[0], q_ref.shape[1]
    seqs_n = kv_ref.shape[0]
    devices_n = frames_n * seqs_n
    me = lax.axis_index("seq")
    head = HEAD_WIDTH
    q_rows = frames_n * sub
    keys_n = seq_step * frames_n * sub
    rows = group * q_rows
    ones = jnp.ones((keys_n, head), jnp.bfloat16)

    def tile(h, q, state, kb, sg, diagonal, qb):
        m, acc = state
        at = pl.ds(pl.multiple_of(kb * sub, sub), sub)
        seqs = pl.ds(sg * seq_step, seq_step)
        k = kv_ref[seqs, :, at, h * head : (h + 1) * head].reshape(keys_n, head)
        v = kv_ref[seqs, :, at, (kv_heads + h) * head : (kv_heads + h + 1) * head]
        v = jnp.concatenate([v.reshape(keys_n, head), ones], axis=1)
        s = lax.dot_general(q, k, (((1,), (1,)), ((), ())), preferred_element_type=jnp.float32)
        if diagonal:
            qi = lax.broadcasted_iota(jnp.int32, (rows, 1), 0) % q_rows
            qpos = (qi % sub) * devices_n + (qi // sub) * seqs_n + me
            ki = lax.broadcasted_iota(jnp.int32, (1, keys_n), 1)
            kpos = (ki % sub) * devices_n + (ki // sub % frames_n) * seqs_n
            kpos = kpos + ki // (sub * frames_n) + sg * seq_step
            s = jnp.where(kpos <= qpos, s, masked_score)
        new = jnp.maximum(m, jnp.max(s, axis=1, keepdims=True))
        e = jnp.exp2(s - new).astype(jnp.bfloat16)
        acc = acc * jnp.exp2(m - new) + dot32(e, v)
        return new, acc

    def one_block(qb, carry):
        at = pl.ds(pl.multiple_of(qb * sub, sub), sub)
        qs = []
        for h in range(kv_heads):
            parts = [
                q_ref[:, at, (h * group + g) * head : (h * group + g + 1) * head].reshape(q_rows, head)
                for g in range(group)
            ]
            qs.append(jnp.concatenate(parts, axis=0))
        steps = seqs_n // seq_step
        state = tuple(
            (jnp.full((rows, 1), masked_score, jnp.float32), jnp.zeros((rows, 2 * head), jnp.float32))
            for _ in range(kv_heads)
        )

        def diag_step(sg, st):
            return tuple(tile(h, qs[h], st[h], qb, sg, True, qb) for h in range(kv_heads))

        state = diag_step(0, state) if steps == 1 else lax.fori_loop(0, steps, diag_step, state)

        def full_step(i, st):
            return tuple(
                tile(h, qs[h], st[h], i // steps, i % steps, False, qb) for h in range(kv_heads)
            )

        state = lax.fori_loop(0, qb * steps, full_step, state)
        for h in range(kv_heads):
            m, acc = state[h]
            out = (acc[:, :head] / acc[:, head:]).astype(jnp.bfloat16)
            for g in range(group):
                piece = out[g * q_rows : (g + 1) * q_rows].reshape(frames_n, sub, head)
                o_ref[:, at, (h * group + g) * head : (h * group + g + 1) * head] = piece
        return carry

    lax.fori_loop(0, own_rows // sub, one_block, 0)


def text_attention(q, kv, kv_heads, group):
    frames_n, own_rows, width = q.shape
    seqs_n = kv.shape[0]
    sub = math.gcd(own_rows, 32)
    seq_step = math.gcd(seqs_n, max(1, 1024 // (sub * frames_n)))
    return pl.pallas_call(
        functools.partial(
            text_kernel, kv_heads=kv_heads, group=group, sub=sub, seq_step=seq_step
        ),
        in_specs=[pl.BlockSpec(memory_space=pltpu.VMEM)] * 2,
        out_specs=pl.BlockSpec(memory_space=pltpu.VMEM),
        out_shape=jax.ShapeDtypeStruct(q.shape, jnp.bfloat16),
        compiler_params=pltpu.CompilerParams(vmem_limit_bytes=50 * 1024 * 1024),
        name="text_attention",
    )(q, kv)


def rotate(values, cosine, sine):
    half = HEAD_WIDTH // 2
    first, second = values[..., :half], values[..., half:]
    return jnp.concatenate(
        [first * cosine - second * sine, second * cosine + first * sine], axis=-1
    )


def per_device(
    vit_states,
    frame_slot,
    patch_count,
    vis_start,
    text_embed,
    vit_ln_gain,
    vit_ln_bias,
    vit_qkv_w,
    vit_qkv_b,
    vit_out_w,
    vit_out_b,
    proj_w,
    proj_b,
    attn_gain,
    wq,
    wk,
    wv,
    wo,
):
    frames_n = lax.axis_size("frame")
    seqs_n = lax.axis_size("seq")
    chips = frames_n // 2
    devices_n = frames_n * seqs_n
    me = lax.axis_index("frame")
    my_seq = lax.axis_index("seq")
    slots_held, frame_max, width_vit = vit_states.shape
    vis_max = frame_max // 4
    own_rows, model_width = text_embed.shape[0], text_embed.shape[2]
    head_size = width_vit // VHEADS
    my_heads = VHEADS // frames_n
    cols = width_vit // frames_n

    w_parts = [
        lax.dynamic_slice_in_dim(vit_qkv_w, i * width_vit + me * cols, cols, 1) for i in range(3)
    ]
    w_parts.append(lax.dynamic_slice_in_dim(vit_out_w, me * cols, cols, 1))
    weights = lax.all_gather(jnp.concatenate(w_parts, 1), "seq", axis=0, tiled=True)
    qkv_bias = [
        lax.dynamic_slice_in_dim(vit_qkv_b, i * width_vit + me * cols, cols, 0) for i in range(3)
    ]
    out_bias = lax.dynamic_slice_in_dim(vit_out_b, me * cols, cols, 0)

    frame_ids = jnp.arange(frame_slot.shape[0])
    holder = frame_slot // slots_held
    holder_frame = holder // seqs_n
    pair_low = (holder_frame - holder_frame % 2) * seqs_n + holder % seqs_n
    pair_order = holder_frame % 2 * slots_held + frame_slot % slots_held
    same_pair = pair_low[:, None] == pair_low[None, :]
    earlier = pair_order[None, :] < pair_order[:, None]
    pair_rank = jnp.sum((same_pair & earlier).astype(jnp.int32), axis=1)
    source_frame = pair_low // seqs_n + pair_rank
    source_seq = pair_low % seqs_n
    mine_low = (source_seq == my_seq) & (pair_low // seqs_n == me - me % 2)
    orders = [
        jnp.sum(jnp.where(mine_low & (pair_rank == (me % 2 ^ i)), pair_order, 0)) for i in range(2)
    ]
    group_hit = (source_frame[None, :] == jnp.arange(frames_n)[:, None]) & (
        source_seq == my_seq
    )[None, :]
    group_count = jnp.sum(jnp.where(group_hit, patch_count[None, :], 0), axis=1)
    group_start = jnp.sum(jnp.where(group_hit, vis_start[None, :], 0), axis=1)

    partner = from_relative(vit_states, 0, 1)
    low_side = me % 2 == 0
    four = jnp.where(
        low_side,
        jnp.concatenate([vit_states, partner], 0),
        jnp.concatenate([partner, vit_states], 0),
    )
    own_state = lax.dynamic_index_in_dim(four, orders[0], 0, keepdims=False)
    pair_state = lax.dynamic_index_in_dim(four, orders[1], 0, keepdims=False)
    parts = [own_state, pair_state]
    for dx in range(1, chips):
        other = from_relative(own_state, dx, 0)
        parts += [other, from_relative(other, 0, 1)]
    states = to_absolute(parts)

    text_own, parts_kept = lax.optimization_barrier(
        (text_embed.reshape(own_rows, model_width), parts[-1])
    )
    text_parts = gather_relative(text_own)
    text_rows = to_absolute(text_parts).reshape(frames_n * own_rows, model_width)

    pieces = 4
    piece_rows = wo.shape[0] // pieces
    wo_pieces = [wo[i * piece_rows : (i + 1) * piece_rows] for i in range(pieces)]
    first_piece, unused = lax.optimization_barrier((wo_pieces[0], text_parts[-1]))
    wo_gathered = [gather_relative(first_piece)]

    wide = states.reshape(frames_n * frame_max, width_vit).astype(jnp.float32)
    average = jnp.mean(wide, axis=1, keepdims=True)
    centred = wide - average
    spread = jnp.mean(centred * centred, axis=1, keepdims=True)
    normed = (centred * lax.rsqrt(spread + vit_epsilon) * vit_ln_gain + vit_ln_bias).astype(
        jnp.bfloat16
    )
    pool = (jnp.arange(frame_max)[None, :] // 4 == jnp.arange(vis_max)[:, None]) * 0.25
    own_columns = lax.dynamic_slice_in_dim(states, me * cols, cols, 2)
    pooled_states = jnp.einsum(
        "pm,fmd->fpd", pool.astype(jnp.bfloat16), own_columns, preferred_element_type=jnp.float32
    )
    qkv = [
        (dot32(normed, weights[:, i * cols : (i + 1) * cols]) + qkv_bias[i])
        .astype(jnp.bfloat16)
        .reshape(frames_n, frame_max, cols)
        for i in range(3)
    ]
    context = vit_attention(group_count, *qkv, my_heads, head_size)
    context_all = to_absolute(gather_relative(context.reshape(frames_n * vis_max, cols)))
    attended = jnp.einsum(
        "gtc,gcd->td",
        context_all,
        weights[:, 3 * cols :].reshape(frames_n, cols, cols),
        preferred_element_type=jnp.float32,
    ).reshape(frames_n, vis_max, cols)
    pooled = (pooled_states + attended + out_bias).astype(jnp.bfloat16)

    laps = vis_max // seqs_n
    dest = jnp.arange(seqs_n)
    token = (
        jnp.mod(dest[None, :, None] - group_start[:, None, None], seqs_n)
        + jnp.arange(laps)[None, None, :] * seqs_n
    )
    pick = (
        token.reshape(frames_n, seqs_n * laps)[:, :, None] == jnp.arange(vis_max)[None, None, :]
    ).astype(jnp.bfloat16)
    routed = jnp.einsum("got,gtd->god", pick, pooled, preferred_element_type=jnp.float32)
    routed = routed.astype(jnp.bfloat16).reshape(frames_n, seqs_n, laps, cols)
    routed = jnp.transpose(routed, (1, 0, 2, 3)).reshape(1, seqs_n, frames_n * laps, cols)
    outgoing = jnp.broadcast_to(routed, (frames_n, seqs_n, frames_n * laps, cols))
    arrived = lax.all_to_all(
        outgoing.reshape(devices_n, frames_n * laps, cols),
        ("frame", "seq"),
        split_axis=0,
        concat_axis=0,
        tiled=True,
    )
    arrived, later = lax.optimization_barrier((arrived, tuple(wo_pieces[1:])))
    for piece in later:
        wo_gathered.append(gather_relative(piece))
    table = jnp.transpose(
        arrived.reshape(frames_n, seqs_n * frames_n * laps, cols), (1, 0, 2)
    ).reshape(seqs_n * frames_n * laps, width_vit)
    visual = (dot32(table, proj_w) + proj_b).astype(jnp.bfloat16)

    group_rows = frames_n * own_rows
    row_ids = jnp.arange(group_rows)
    positions = row_ids % own_rows * devices_n + row_ids // own_rows * seqs_n + my_seq
    token_frame = positions // own_rows
    frame_hot = token_frame[:, None] == frame_ids[None, :]

    def of_frame(values):
        return jnp.sum(jnp.where(frame_hot, values[None, :], 0), axis=1)

    within = positions - of_frame(vis_start)
    is_visual = (within >= 0) & (within < of_frame(patch_count) // 4)
    table_row = of_frame(source_seq * frames_n + source_frame) * laps + within // seqs_n
    table_hot = (is_visual[:, None] & (table_row[:, None] == jnp.arange(table.shape[0])[None, :]))
    fetched = dot32(table_hot.astype(jnp.bfloat16), visual)
    merged = jnp.where(is_visual[:, None], fetched, text_rows.astype(jnp.float32))
    normed_tok = (
        merged
        * lax.rsqrt(jnp.mean(merged * merged, axis=1, keepdims=True) + norm_epsilon)
        * attn_gain
    ).astype(jnp.bfloat16)

    query_width, kv_width = wq.shape[1], wk.shape[1]
    kv_heads = kv_width // HEAD_WIDTH
    query_heads = query_width // HEAD_WIDTH
    exponents = jnp.arange(0, HEAD_WIDTH, 2).astype(jnp.float32) / HEAD_WIDTH
    inverse = jnp.power(jnp.float32(rope_theta), -exponents)
    angles = (positions.astype(jnp.float32)[:, None] * inverse[None, :])[:, None, :]
    cosine, sine = jnp.cos(angles), jnp.sin(angles)
    keys = rotate(dot32(normed_tok, wk).reshape(group_rows, kv_heads, HEAD_WIDTH), cosine, sine)
    values = dot32(normed_tok, wv)
    own_kv = jnp.concatenate(
        [keys.reshape(group_rows, kv_width).astype(jnp.bfloat16), values.astype(jnp.bfloat16)], 1
    )
    kv = lax.all_gather(own_kv, "seq", axis=0, tiled=True)
    scale = LOG2E / math.sqrt(HEAD_WIDTH)
    queries = rotate(
        dot32(normed_tok, wq).reshape(group_rows, query_heads, HEAD_WIDTH),
        cosine * scale,
        sine * scale,
    ).astype(jnp.bfloat16)
    context_tok = text_attention(
        queries.reshape(frames_n, own_rows, query_width),
        kv.reshape(seqs_n, frames_n, own_rows, 2 * kv_width),
        kv_heads,
        query_heads // kv_heads,
    )

    mixed = jnp.zeros((own_rows, wo.shape[1]), jnp.float32)
    for dx in range(chips):
        for dc in range(2):
            to = jnp.mod(me // 2 - dx, chips) * 2 + (me % 2 ^ dc)
            block = lax.dynamic_index_in_dim(context_tok, to, 0, keepdims=False)
            if dx or dc:
                block = from_relative(block, dx, dc)
            for i in range(pieces):
                mixed = mixed + dot32(
                    block[:, i * piece_rows : (i + 1) * piece_rows], wo_gathered[i][dx * 2 + dc]
                )
    return mixed.astype(jnp.bfloat16).reshape(own_rows, 1, wo.shape[1])


def solution(mesh):
    return jax.shard_map(
        per_device,
        mesh=mesh,
        in_specs=(
            P(("frame", "seq"), None, None),
            P(),
            P(),
            P(),
            P(None, ("frame", "seq"), None),
            P(),
            P(),
            P("seq", None),
            P(),
            P("seq", None),
            P(),
            P(),
            P(),
            P(),
            P(None, "frame"),
            P(None, "frame"),
            P(None, "frame"),
            P("frame", None),
        ),
        out_specs=P(None, ("frame", "seq"), None),
        check_vma=False,
    )
```

```python
import functools
import math

import jax
import jax.numpy as jnp
from jax import lax
from jax.experimental import pallas as pl
from jax.experimental.layout import Layout, with_layout_constraint
from jax.experimental.pallas import tpu as pltpu
from jax.sharding import PartitionSpec as P

VHEADS = 16
HEAD_WIDTH = 128

rope_theta = 500000.0
vit_epsilon = 1e-06
norm_epsilon = 1e-05
masked_score = -1e30
LOG2E = math.log2(math.e)


def dot32(a, b):
    return jnp.dot(a, b, preferred_element_type=jnp.float32)


def from_relative(value, dx, dc):
    n = lax.axis_size("frame")
    chips = n // 2
    pairs = []
    for dst in range(n):
        src = ((dst // 2 + dx) % chips) * 2 + ((dst % 2) ^ dc)
        pairs.append((src, dst))
    return lax.ppermute(value, "frame", pairs)


def gather_relative(value):
    chips = lax.axis_size("frame") // 2
    out = []
    for dx in range(chips):
        same = value if dx == 0 else from_relative(value, dx, 0)
        out.append(same)
        out.append(from_relative(same, 0, 1))
    return out


def to_absolute(parts):
    n = len(parts)
    chips = n // 2
    me = lax.axis_index("frame")
    stack = jnp.stack(parts)
    out = []
    for g in range(n):
        dx = jnp.mod(g // 2 - me // 2, chips)
        dc = (g % 2) ^ (me % 2)
        out.append(lax.dynamic_index_in_dim(stack, dx * 2 + dc, 0, keepdims=False))
    return jnp.stack(out)


def vit_kernel(count_ref, q_ref, k_ref, v_ref, o_ref, *, heads, head_size):
    frame = pl.program_id(0)
    rows, width = q_ref.shape[1], q_ref.shape[2]
    q = q_ref[0]
    k = k_ref[0]
    v = v_ref[0]
    count = count_ref[frame]
    column = lax.broadcasted_iota(jnp.int32, (rows, rows), 1)
    live = column < count
    lane = lax.broadcasted_iota(jnp.int32, (rows, width), 1)
    zero = jnp.zeros((), q.dtype)
    total = jnp.zeros((rows, width), jnp.float32)
    for h in range(heads):
        mine = (lane >= h * head_size) & (lane < (h + 1) * head_size)
        qh = jnp.where(mine, q, zero)
        s = lax.dot_general(qh, k, (((1,), (1,)), ((), ())), preferred_element_type=jnp.float32)
        s = jnp.where(live, s * (1.0 / math.sqrt(head_size)), masked_score)
        e = jnp.exp(s - jnp.max(s, axis=1, keepdims=True))
        p = (e / jnp.sum(e, axis=1, keepdims=True)).astype(jnp.bfloat16)
        vh = jnp.where(mine, v, zero)
        total = total + dot32(p, vh)
    context = total.astype(jnp.bfloat16)
    out_rows = o_ref.shape[1]
    pr = lax.broadcasted_iota(jnp.int32, (out_rows, rows), 0)
    pc = lax.broadcasted_iota(jnp.int32, (out_rows, rows), 1)
    pool = jnp.where(pc // 4 == pr, 0.25, 0.0).astype(jnp.bfloat16)
    o_ref[0] = dot32(pool, context).astype(jnp.bfloat16)


def vit_attention(counts, q, k, v, heads, head_size):
    frames, rows, width = q.shape
    block = pl.BlockSpec((1, rows, width), lambda i: (i, 0, 0))
    return pl.pallas_call(
        functools.partial(vit_kernel, heads=heads, head_size=head_size),
        grid=(frames,),
        in_specs=[pl.BlockSpec(memory_space=pltpu.SMEM), block, block, block],
        out_specs=pl.BlockSpec((1, rows // 4, width), lambda i: (i, 0, 0)),
        out_shape=jax.ShapeDtypeStruct((frames, rows // 4, width), jnp.bfloat16),
        cost_estimate=pl.CostEstimate(
            flops=4 * frames * rows * rows * width * heads,
            bytes_accessed=6 * q.size,
            transcendentals=frames * heads * rows * rows,
        ),
        name="vit_attention",
    )(counts, q, k, v)


def text_kernel(q_ref, kv_ref, o_ref, *, kv_heads, group, sub, seq_step):
    frames_n, own_rows = q_ref.shape[0], q_ref.shape[1]
    seqs_n = kv_ref.shape[0]
    devices_n = frames_n * seqs_n
    me = lax.axis_index("seq")
    head = HEAD_WIDTH
    q_rows = frames_n * sub
    keys_n = seq_step * frames_n * sub
    rows = group * q_rows
    ones = jnp.ones((keys_n, head), jnp.bfloat16)

    def tile(h, q, state, kb, sg, diagonal, qb):
        m, acc = state
        at = pl.ds(pl.multiple_of(kb * sub, sub), sub)
        seqs = pl.ds(sg * seq_step, seq_step)
        k = kv_ref[seqs, :, at, h * head : (h + 1) * head].reshape(keys_n, head)
        v = kv_ref[seqs, :, at, (kv_heads + h) * head : (kv_heads + h + 1) * head]
        v = jnp.concatenate([v.reshape(keys_n, head), ones], axis=1)
        s = lax.dot_general(q, k, (((1,), (1,)), ((), ())), preferred_element_type=jnp.float32)
        if diagonal:
            qi = lax.broadcasted_iota(jnp.int32, (rows, 1), 0) % q_rows
            qpos = (qi % sub) * devices_n + (qi // sub) * seqs_n + me
            ki = lax.broadcasted_iota(jnp.int32, (1, keys_n), 1)
            kpos = (ki % sub) * devices_n + (ki // sub % frames_n) * seqs_n
            kpos = kpos + ki // (sub * frames_n) + sg * seq_step
            s = jnp.where(kpos <= qpos, s, masked_score)
        new = jnp.maximum(m, jnp.max(s, axis=1, keepdims=True))
        e = jnp.exp2(s - new).astype(jnp.bfloat16)
        acc = acc * jnp.exp2(m - new) + dot32(e, v)
        return new, acc

    def one_block(qb, carry):
        at = pl.ds(pl.multiple_of(qb * sub, sub), sub)
        qs = []
        for h in range(kv_heads):
            parts = [
                q_ref[:, at, (h * group + g) * head : (h * group + g + 1) * head].reshape(q_rows, head)
                for g in range(group)
            ]
            qs.append(jnp.concatenate(parts, axis=0))
        steps = seqs_n // seq_step
        state = tuple(
            (jnp.full((rows, 1), masked_score, jnp.float32), jnp.zeros((rows, 2 * head), jnp.float32))
            for _ in range(kv_heads)
        )

        def diag_step(sg, st):
            return tuple(tile(h, qs[h], st[h], qb, sg, True, qb) for h in range(kv_heads))

        state = diag_step(0, state) if steps == 1 else lax.fori_loop(0, steps, diag_step, state)

        def full_step(i, st):
            return tuple(
                tile(h, qs[h], st[h], i // steps, i % steps, False, qb) for h in range(kv_heads)
            )

        state = lax.fori_loop(0, qb * steps, full_step, state)
        for h in range(kv_heads):
            m, acc = state[h]
            out = (acc[:, :head] / acc[:, head:]).astype(jnp.bfloat16)
            for g in range(group):
                piece = out[g * q_rows : (g + 1) * q_rows].reshape(frames_n, sub, head)
                o_ref[:, at, (h * group + g) * head : (h * group + g + 1) * head] = piece
        return carry

    lax.fori_loop(0, own_rows // sub, one_block, 0)


def text_attention(q, kv, kv_heads, group):
    frames_n, own_rows, width = q.shape
    seqs_n = kv.shape[0]
    sub = math.gcd(own_rows, 32)
    seq_step = math.gcd(seqs_n, max(1, 1024 // (sub * frames_n)))
    return pl.pallas_call(
        functools.partial(
            text_kernel, kv_heads=kv_heads, group=group, sub=sub, seq_step=seq_step
        ),
        in_specs=[pl.BlockSpec(memory_space=pltpu.VMEM)] * 2,
        out_specs=pl.BlockSpec(memory_space=pltpu.VMEM),
        out_shape=jax.ShapeDtypeStruct(q.shape, jnp.bfloat16),
        compiler_params=pltpu.CompilerParams(vmem_limit_bytes=50 * 1024 * 1024),
        cost_estimate=pl.CostEstimate(
            flops=4 * seqs_n * frames_n * own_rows * frames_n * own_rows * width,
            bytes_accessed=4 * q.size + 2 * kv.size,
            transcendentals=0,
        ),
        name="text_attention",
    )(q, kv)


def mix_kernel(*refs, groups, pieces):
    blocks, weights, o_ref = refs[:groups], refs[groups:-1], refs[-1]
    total = jnp.zeros(o_ref.shape, jnp.float32)
    for g in range(groups):
        for i in range(pieces):
            w = weights[g * pieces + i]
            depth = w.shape[0]
            total = total + dot32(blocks[g][:, i * depth : (i + 1) * depth], w[...])
    o_ref[...] = total.astype(o_ref.dtype)


def mix(blocks, weights):
    rows, depth = blocks[0].shape
    out_cols = weights[0].shape[1]
    step = math.gcd(out_cols, 512)
    whole = pl.BlockSpec((rows, depth), lambda j: (0, 0))
    column = pl.BlockSpec((weights[0].shape[0], step), lambda j: (0, j))
    return pl.pallas_call(
        functools.partial(
            mix_kernel, groups=len(blocks), pieces=len(weights) // len(blocks)
        ),
        grid=(out_cols // step,),
        in_specs=[whole] * len(blocks) + [column] * len(weights),
        out_specs=pl.BlockSpec((rows, step), lambda j: (0, j)),
        out_shape=jax.ShapeDtypeStruct((rows, out_cols), jnp.bfloat16),
        name="mix",
    )(*blocks, *weights)


def rotate(values, cosine, sine):
    half = HEAD_WIDTH // 2
    first, second = values[..., :half], values[..., half:]
    return jnp.concatenate(
        [first * cosine - second * sine, second * cosine + first * sine], axis=-1
    )


def per_device(
    vit_states,
    frame_slot,
    patch_count,
    vis_start,
    text_embed,
    vit_ln_gain,
    vit_ln_bias,
    vit_qkv_w,
    vit_qkv_b,
    vit_out_w,
    vit_out_b,
    proj_w,
    proj_b,
    attn_gain,
    wq,
    wk,
    wv,
    wo,
):
    frames_n = lax.axis_size("frame")
    seqs_n = lax.axis_size("seq")
    chips = frames_n // 2
    devices_n = frames_n * seqs_n
    me = lax.axis_index("frame")
    my_seq = lax.axis_index("seq")
    slots_held, frame_max, width_vit = vit_states.shape
    vis_max = frame_max // 4
    own_rows, model_width = text_embed.shape[0], text_embed.shape[2]
    head_size = width_vit // VHEADS
    my_heads = VHEADS // frames_n
    cols = width_vit // frames_n

    w_parts = [
        lax.dynamic_slice_in_dim(vit_qkv_w, i * width_vit + me * cols, cols, 1) for i in range(3)
    ]
    weights = lax.all_gather(jnp.concatenate(w_parts, 1), "seq", axis=0, tiled=True)
    out_own = lax.dynamic_slice_in_dim(vit_out_w, me * cols, cols, 1)
    wanted = -(-(1 << 20) // (2 * width_vit * HEAD_WIDTH)) * HEAD_WIDTH
    out_own = jnp.pad(out_own, ((0, 0), (0, max(0, wanted - cols))))
    out_own, weights = lax.optimization_barrier((out_own, weights))
    out_weights = lax.all_gather(out_own, "seq", axis=0, tiled=True)
    qkv_bias = [
        lax.dynamic_slice_in_dim(vit_qkv_b, i * width_vit + me * cols, cols, 0) for i in range(3)
    ]
    out_bias = lax.dynamic_slice_in_dim(vit_out_b, me * cols, cols, 0)

    frame_ids = jnp.arange(frame_slot.shape[0])
    holder = frame_slot // slots_held
    holder_frame = holder // seqs_n
    pair_low = (holder_frame - holder_frame % 2) * seqs_n + holder % seqs_n
    pair_order = holder_frame % 2 * slots_held + frame_slot % slots_held
    same_pair = pair_low[:, None] == pair_low[None, :]
    earlier = pair_order[None, :] < pair_order[:, None]
    pair_rank = jnp.sum((same_pair & earlier).astype(jnp.int32), axis=1)
    source_frame = pair_low // seqs_n + pair_rank
    source_seq = pair_low % seqs_n
    mine_low = (source_seq == my_seq) & (pair_low // seqs_n == me - me % 2)
    orders = [
        jnp.sum(jnp.where(mine_low & (pair_rank == (me % 2 ^ i)), pair_order, 0)) for i in range(2)
    ]
    group_hit = (source_frame[None, :] == jnp.arange(frames_n)[:, None]) & (
        source_seq == my_seq
    )[None, :]
    group_count = jnp.sum(jnp.where(group_hit, patch_count[None, :], 0), axis=1)
    group_start = jnp.sum(jnp.where(group_hit, vis_start[None, :], 0), axis=1)

    partner = from_relative(vit_states, 0, 1)
    low_side = me % 2 == 0
    four = jnp.where(
        low_side,
        jnp.concatenate([vit_states, partner], 0),
        jnp.concatenate([partner, vit_states], 0),
    )
    own_state = lax.dynamic_index_in_dim(four, orders[0], 0, keepdims=False)
    pair_state = lax.dynamic_index_in_dim(four, orders[1], 0, keepdims=False)
    parts = [own_state, pair_state]
    for dx in range(1, chips):
        other = from_relative(own_state, dx, 0)
        parts += [other, from_relative(other, 0, 1)]
    states = to_absolute(parts)

    piece_rows = math.gcd(wo.shape[0], HEAD_WIDTH)
    pieces = wo.shape[0] // piece_rows
    wo_pieces = [wo[i * piece_rows : (i + 1) * piece_rows] for i in range(pieces)]
    text_own, last_part = lax.optimization_barrier(
        (text_embed.reshape(own_rows, model_width), parts[-1])
    )
    text_parts = gather_relative(text_own)

    wide = states.reshape(frames_n * frame_max, width_vit).astype(jnp.float32)
    average = jnp.mean(wide, axis=1, keepdims=True)
    first_piece, average = lax.optimization_barrier((wo_pieces[0], average))
    first_across = [first_piece]
    for dx in range(1, chips):
        first_across.append(from_relative(first_piece, dx, 0))
    centred = wide - average
    spread = jnp.mean(centred * centred, axis=1, keepdims=True)
    normed = (centred * lax.rsqrt(spread + vit_epsilon) * vit_ln_gain + vit_ln_bias).astype(
        jnp.bfloat16
    )
    pool = (jnp.arange(frame_max)[None, :] // 4 == jnp.arange(vis_max)[:, None]) * 0.25
    own_columns = lax.dynamic_slice_in_dim(states, me * cols, cols, 2)
    pooled_states = jnp.einsum(
        "pm,fmd->fpd", pool.astype(jnp.bfloat16), own_columns, preferred_element_type=jnp.float32
    )
    projected = (dot32(normed, weights) + jnp.concatenate(qkv_bias)).astype(jnp.bfloat16)
    projected = with_layout_constraint(projected, Layout((0, 1)))
    qkv = [
        projected[:, i * cols : (i + 1) * cols].reshape(frames_n, frame_max, cols)
        for i in range(3)
    ]
    context = vit_attention(group_count, *qkv, my_heads, head_size)
    context, text_parts, first_across = lax.optimization_barrier(
        (context, text_parts, first_across)
    )
    first_parts = []
    for same in first_across:
        first_parts += [same, from_relative(same, 0, 1)]
    wo_gathered = [first_parts]
    text_rows = to_absolute(text_parts).reshape(frames_n * own_rows, model_width)
    context_all = to_absolute(gather_relative(context.reshape(frames_n * vis_max, cols)))
    attended = jnp.einsum(
        "gtc,gcd->td",
        context_all,
        out_weights[:, :cols].reshape(frames_n, cols, cols),
        preferred_element_type=jnp.float32,
    ).reshape(frames_n, vis_max, cols)
    pooled = (pooled_states + attended + out_bias).astype(jnp.bfloat16)

    laps = vis_max // seqs_n
    dest = jnp.arange(seqs_n)
    token = (
        jnp.mod(dest[None, :, None] - group_start[:, None, None], seqs_n)
        + jnp.arange(laps)[None, None, :] * seqs_n
    )
    pick = (
        token.reshape(frames_n, seqs_n * laps)[:, :, None] == jnp.arange(vis_max)[None, None, :]
    ).astype(jnp.bfloat16)
    routed = jnp.einsum("got,gtd->god", pick, pooled, preferred_element_type=jnp.float32)
    routed = routed.astype(jnp.bfloat16).reshape(frames_n, seqs_n, laps, cols)
    routed = jnp.transpose(routed, (1, 0, 2, 3)).reshape(1, seqs_n, frames_n * laps, cols)
    outgoing = jnp.broadcast_to(routed, (frames_n, seqs_n, frames_n * laps, cols))
    arrived = lax.all_to_all(
        outgoing.reshape(devices_n, frames_n * laps, cols),
        ("frame", "seq"),
        split_axis=0,
        concat_axis=0,
        tiled=True,
    )
    arrived, later = lax.optimization_barrier((arrived, tuple(wo_pieces[1:])))
    for piece in later:
        wo_gathered.append(gather_relative(piece))
    table = jnp.transpose(
        arrived.reshape(frames_n, seqs_n * frames_n * laps, cols), (1, 0, 2)
    ).reshape(seqs_n * frames_n * laps, width_vit)
    visual = (dot32(table, proj_w) + proj_b).astype(jnp.bfloat16)

    group_rows = frames_n * own_rows
    row_ids = jnp.arange(group_rows)
    positions = row_ids % own_rows * devices_n + row_ids // own_rows * seqs_n + my_seq
    token_frame = positions // own_rows
    frame_hot = token_frame[:, None] == frame_ids[None, :]

    def of_frame(values):
        return jnp.sum(jnp.where(frame_hot, values[None, :], 0), axis=1)

    within = positions - of_frame(vis_start)
    is_visual = (within >= 0) & (within < of_frame(patch_count) // 4)
    table_row = of_frame(source_seq * frames_n + source_frame) * laps + within // seqs_n
    table_hot = (is_visual[:, None] & (table_row[:, None] == jnp.arange(table.shape[0])[None, :]))
    fetched = dot32(table_hot.astype(jnp.bfloat16), visual)
    merged = jnp.where(is_visual[:, None], fetched, text_rows.astype(jnp.float32))
    normed_tok = (
        merged
        * lax.rsqrt(jnp.mean(merged * merged, axis=1, keepdims=True) + norm_epsilon)
        * attn_gain
    ).astype(jnp.bfloat16)

    query_width, kv_width = wq.shape[1], wk.shape[1]
    kv_heads = kv_width // HEAD_WIDTH
    query_heads = query_width // HEAD_WIDTH
    exponents = jnp.arange(0, HEAD_WIDTH, 2).astype(jnp.float32) / HEAD_WIDTH
    inverse = jnp.power(jnp.float32(rope_theta), -exponents)
    angles = (positions.astype(jnp.float32)[:, None] * inverse[None, :])[:, None, :]
    cosine, sine = jnp.cos(angles), jnp.sin(angles)
    keys = rotate(dot32(normed_tok, wk).reshape(group_rows, kv_heads, HEAD_WIDTH), cosine, sine)
    values = dot32(normed_tok, wv)
    own_kv = jnp.concatenate(
        [keys.reshape(group_rows, kv_width).astype(jnp.bfloat16), values.astype(jnp.bfloat16)], 1
    )
    own_kv = with_layout_constraint(own_kv, Layout((0, 1)))
    kv = lax.all_gather(own_kv, "seq", axis=0, tiled=True)
    scale = LOG2E / math.sqrt(HEAD_WIDTH)
    queries = rotate(
        dot32(normed_tok, wq).reshape(group_rows, query_heads, HEAD_WIDTH),
        cosine * scale,
        sine * scale,
    ).astype(jnp.bfloat16)
    context_tok = text_attention(
        queries.reshape(frames_n, own_rows, query_width),
        kv.reshape(seqs_n, frames_n, own_rows, 2 * kv_width),
        kv_heads,
        query_heads // kv_heads,
    )

    blocks, mix_weights = [], []
    for dx in range(chips):
        for dc in range(2):
            to = jnp.mod(me // 2 - dx, chips) * 2 + (me % 2 ^ dc)
            block = lax.dynamic_index_in_dim(context_tok, to, 0, keepdims=False)
            if dx or dc:
                block = from_relative(block, dx, dc)
            blocks.append(block)
            mix_weights += [wo_gathered[i][dx * 2 + dc] for i in range(pieces)]
    mixed = mix(blocks, mix_weights)
    return mixed.reshape(own_rows, 1, wo.shape[1])


def solution(mesh):
    return jax.shard_map(
        per_device,
        mesh=mesh,
        in_specs=(
            P(("frame", "seq"), None, None),
            P(),
            P(),
            P(),
            P(None, ("frame", "seq"), None),
            P(),
            P(),
            P("seq", None),
            P(),
            P("seq", None),
            P(),
            P(),
            P(),
            P(),
            P(None, "frame"),
            P(None, "frame"),
            P(None, "frame"),
            P("frame", None),
        ),
        out_specs=P(None, ("frame", "seq"), None),
        check_vma=False,
    )
```
